32 devices in a mesh: section: 4 (over x, core), dp: 8 (over z, y).
Axes of the slice: x: 2, y: 2, z: 4, core: 2. Of those that a mesh axis runs over, the one named last changes fastest.
Arguments:
- clean_latent: float32 [64, 256], P('dp'), may hold values from -6 to 6
- noise_draw: float32 [64, 256], P('dp'), may hold values from -6 to 6
- step_index: int32 [64], P('dp'), may hold values from 250 to 1000
- labels: int32 [64], P('dp'), may hold values from 0 to 999
- guide_level: int32 [64], P('dp'), may hold values from 0 to 8
- class_table: bfloat16 [1001, 1152], replicated, may hold values from -6 to 6
- embed_in: bfloat16 [16, 1152], replicated, may hold values from -1.5 to 1.5
- embed_out: bfloat16 [1152, 16], replicated, may hold values from -0.1875 to 0.1875
- teacher_up: bfloat16 [4, 1152, 2304], P('section', 'dp'), may hold values from -0.1875 to 0.1875
- teacher_down: bfloat16 [4, 2304, 1152], P('section', 'dp'), may hold values from -0.125 to 0.125
- teacher_gain: float32 [4, 3, 1152], P('section'), may hold values from -3 to 3
- teacher_bias: float32 [4, 3, 1152], P('section'), may hold values from -3 to 3
- student_up: bfloat16 [1152, 4608], P(None, 'section'), may hold values from -0.1875 to 0.1875
- student_down: bfloat16 [4608, 1152], P('section'), may hold values from -0.09375 to 0.09375
- student_gain: float32 [3, 1152], replicated, may hold values from -3 to 3
- student_bias: float32 [3, 1152], replicated, may hold values from -3 to 3
- guide_vec: float32 [1152], replicated, may hold values from -3 to 3
Outputs:
- distill_target: float32 [64, 256], P('dp')
- grad_up: float32 [1152, 4608], P('dp', 'section')
- grad_down: float32 [4608, 1152], P(('section', 'dp'))
The draws below stay inside these ranges and needn't reach their ends.
All inputs are finite; a program needn't handle non-finite values.
Results may differ from the reference program's by a relative error of at most 0.017.
Values may be sent and summed in bfloat16 or wider, within the bound.
No kernel may reach another device: no remote copies, remote signals or barrier semaphores. Data moves between devices by JAX's collectives and lax.ppermute only.
A program may use at most 128 MiB of HBM per device.

```python
import math
import jax
import jax.numpy as jnp
from jax import lax

D = 1152
FF_T = 2304
FF_S = 4608
CLASSES = 1000
CH = 16
TSTEPS = 1000
STRIDE = 125
SEQ = 16
SECTIONS = 4
SAMPLES = 64


def place_ends(entries, rng, least, largest):
    extent = entries.shape
    place = [jax.random.randint(jax.random.fold_in(rng, axis), (), 0, extent[axis]) for axis in range(len(extent))]
    entries = entries.at[tuple(place)].set(least)
    longest = extent.index(max(extent))
    place[longest] = (place[longest] + 1) % extent[longest]
    return entries.at[tuple(place)].set(largest)


def shard_levels(key, shape, pieces, smallest, high):
    factor_of, own = 1.0, jax.random.fold_in(key, 6)
    for axis_at, blocks in pieces:
        steps = jnp.exp(jax.random.uniform(jax.random.fold_in(own, axis_at), (blocks,), jnp.float32, smallest / len(pieces), high / len(pieces)))
        factor_of = factor_of * jnp.repeat(steps, shape[axis_at] // blocks).reshape([-1 if axis == axis_at else 1 for axis in range(len(shape))])
    return factor_of


def gaussian(own_key, shape, scale, reach, shards=(), held_as=jnp.bfloat16):
    entries = jax.random.normal(own_key, shape, jnp.float32) * scale
    if len(shards) > 0:
        entries = shard_levels(own_key, shape, shards, -0.22, 0.18) * entries
    return jnp.clip(entries, min=-reach, max=reach).astype(held_as)


def setup_inputs(seed: int = 0) -> dict:
    seeds = jax.random.split(jax.random.key(seed), 18)
    return {
        "clean_latent": gaussian(seeds[0], (SAMPLES, SEQ * CH), 1.0, 6.0, ((0, 8),), jnp.float32),
        "noise_draw": gaussian(seeds[1], (SAMPLES, SEQ * CH), 1.0, 6.0, ((0, 8),), jnp.float32),
        "step_index": place_ends(jax.random.randint(seeds[2], (SAMPLES,), 2 * STRIDE, TSTEPS + 1), jax.random.fold_in(seeds[2], 1), 2 * STRIDE, TSTEPS).astype(jnp.int32),
        "labels": place_ends(jax.random.randint(seeds[3], (SAMPLES,), 0, CLASSES), jax.random.fold_in(seeds[3], 1), 0, CLASSES - 1).astype(jnp.int32),
        "guide_level": place_ends(jax.random.randint(seeds[4], (SAMPLES,), 0, 9), jax.random.fold_in(seeds[4], 1), 0, 8).astype(jnp.int32),
        "class_table": gaussian(seeds[5], (CLASSES + 1, D), 1.0, 6.0),
        "embed_in": gaussian(seeds[6], (CH, D), CH ** -0.5, 1.5),
        "embed_out": gaussian(seeds[7], (D, CH), D ** -0.5, 0.1875),
        "teacher_up": gaussian(seeds[8], (SECTIONS, D, FF_T), D ** -0.5, 0.1875, ((0, 4), (1, 8))),
        "teacher_down": gaussian(seeds[9], (SECTIONS, FF_T, D), FF_T ** -0.5, 0.125, ((0, 4), (1, 8))),
        "teacher_gain": gaussian(seeds[10], (SECTIONS, 3, D), 0.5, 3.0, ((0, 4),), jnp.float32),
        "teacher_bias": gaussian(seeds[11], (SECTIONS, 3, D), 0.5, 3.0, ((0, 4),), jnp.float32),
        "student_up": gaussian(seeds[12], (D, FF_S), D ** -0.5, 0.1875, ((1, 4),)),
        "student_down": gaussian(seeds[13], (FF_S, D), FF_S ** -0.5, 0.09375, ((0, 4),)),
        "student_gain": gaussian(seeds[14], (3, D), 0.5, 3.0, (), jnp.float32),
        "student_bias": gaussian(seeds[15], (3, D), 0.5, 3.0, (), jnp.float32),
        "guide_vec": gaussian(seeds[16], (D,), 0.5, 3.0, (), jnp.float32),
    }


norm_eps = 1e-06

def layer_norm(values):
    center = values - lax.optimization_barrier(jnp.mean(values, axis=-1, keepdims=True))
    spread = lax.optimization_barrier(jnp.mean(center * center, axis=-1, keepdims=True))
    return center * lax.rsqrt(spread + norm_eps)

def sinusoid(step_ids, model_width):
    half_width = model_width // 2
    frequency = jnp.exp(-math.log(10000.0) * jnp.arange(half_width, dtype=jnp.float32) / half_width)
    phase_arg = step_ids.astype(jnp.float32)[:, None] * frequency[None, :]
    return jnp.concatenate([jnp.cos(phase_arg), jnp.sin(phase_arg)], axis=-1)

def plan(step_ids):
    angle_t = 0.5 * math.pi / TSTEPS * step_ids.astype(jnp.float32)
    return (jnp.cos(angle_t), jnp.sin(angle_t))

def embed_tokens(latent, embed_in):
    leading = latent.shape[0]
    patches = latent.reshape(leading * (latent.shape[1] // CH), CH).astype(jnp.bfloat16)
    tokens = jnp.dot(patches, embed_in, preferred_element_type=jnp.float32)
    return tokens.reshape(leading, latent.shape[1] // CH, embed_in.shape[1]).astype(jnp.bfloat16)

def mlp_block(inputs, modulation, up_proj, down_proj):
    groups, seq_len, model_width = inputs.shape
    residual_in = inputs.astype(jnp.float32)
    shift_rows = modulation[:, 0, None, :]
    scale_rows = modulation[:, 1, None, :]
    gate_rows = modulation[:, 2, None, :]
    normed = (layer_norm(residual_in) * (1.0 + scale_rows) + shift_rows).astype(jnp.bfloat16)
    pre_act = jnp.dot(normed.reshape(groups * seq_len, model_width), up_proj, preferred_element_type=jnp.float32)
    hidden = jax.nn.gelu(pre_act, approximate=True).astype(jnp.bfloat16)
    mixed = jnp.dot(hidden, down_proj, preferred_element_type=jnp.float32).reshape(groups, seq_len, model_width)
    return (residual_in + gate_rows * mixed).astype(jnp.bfloat16)

def velocity(states, embed_out):
    groups, seq_len, model_width = states.shape
    normed = layer_norm(states.astype(jnp.float32)).astype(jnp.bfloat16)
    result = jnp.dot(normed.reshape(groups * seq_len, model_width), embed_out, preferred_element_type=jnp.float32)
    return result.reshape(groups, seq_len * embed_out.shape[1])

def ddim_step(latent, predicted, time_now, time_next):
    alpha_now, sigma_now = plan(time_now)
    alpha_next, sigma_next = plan(time_next)
    clean_est = alpha_now[:, None] * latent - sigma_now[:, None] * predicted
    noise_est = sigma_now[:, None] * latent + alpha_now[:, None] * predicted
    return alpha_next[:, None] * clean_est + sigma_next[:, None] * noise_est

def gelu_slope(pre_act):
    return jax.vjp(lambda inner: jax.nn.gelu(inner, approximate=True), pre_act)[1](jnp.ones_like(pre_act))[0]

def reference(clean_latent, noise_draw, step_index, labels, guide_level, class_table, embed_in, embed_out, teacher_up, teacher_down, teacher_gain, teacher_bias, student_up, student_down, student_gain, student_bias, guide_vec):
    model_width = class_table.shape[1]
    samples = clean_latent.shape[0]
    seq_len = clean_latent.shape[1] // CH
    alpha_t, sigma_t = plan(step_index)
    noised = alpha_t[:, None] * clean_latent + sigma_t[:, None] * noise_draw
    guidance = 0.5 * guide_level.astype(jnp.float32)
    label_rows = jnp.take(class_table, labels, axis=0).astype(jnp.float32)
    null_row = class_table[class_table.shape[0] - 1].astype(jnp.float32)
    first_in = embed_tokens(noised, embed_in)
    latent = noised
    for which_step in range(2):
        time_now = step_index - which_step * STRIDE
        wave_rows = sinusoid(time_now, model_width)
        conditions = jnp.stack([wave_rows + label_rows, wave_rows + null_row[None, :]], axis=1)
        entry_rows = first_in if which_step == 0 else embed_tokens(latent, embed_in)
        states = jnp.stack([entry_rows, entry_rows], axis=1).reshape(samples * 2, seq_len, model_width)
        for layer in range(SECTIONS):
            modulation = conditions[:, :, None, :] * teacher_gain[layer] + teacher_bias[layer]
            states = mlp_block(states, modulation.reshape(samples * 2, 3, model_width), teacher_up[layer], teacher_down[layer])
        predicted = velocity(states, embed_out).reshape(samples, 2, seq_len * CH)
        guided = (1.0 + guidance)[:, None] * predicted[:, 0] - guidance[:, None] * predicted[:, 1]
        latent = ddim_step(latent, guided, time_now, time_now - STRIDE)
    alpha_end, sigma_end = plan(step_index - 2 * STRIDE)
    sigma_ratio = sigma_end / sigma_t
    distill_target = (latent - sigma_ratio[:, None] * noised) / (alpha_end - sigma_ratio * alpha_t)[:, None]
    student_cond = sinusoid(step_index, model_width) + label_rows + guidance[:, None] * guide_vec[None, :]
    modulation = student_cond[:, None, :] * student_gain[None] + student_bias[None]
    shift_rows = modulation[:, 0, None, :]
    scale_rows = modulation[:, 1, None, :]
    gate_rows = modulation[:, 2, None, :]
    row_count = samples * seq_len
    residual_in = first_in.astype(jnp.float32)
    normed = (layer_norm(residual_in) * (1.0 + scale_rows) + shift_rows).astype(jnp.bfloat16).reshape(row_count, model_width)
    pre_act = jnp.dot(normed, student_up, preferred_element_type=jnp.float32)
    hidden = jax.nn.gelu(pre_act, approximate=True).astype(jnp.bfloat16)
    mixed = jnp.dot(hidden, student_down, preferred_element_type=jnp.float32).reshape(samples, seq_len, model_width)
    state_rows = residual_in + gate_rows * mixed
    normed_out, pullback = jax.vjp(layer_norm, state_rows)
    predicted = jnp.dot(normed_out.astype(jnp.bfloat16).reshape(row_count, model_width), embed_out, preferred_element_type=jnp.float32).reshape(samples, seq_len * CH)
    estimate = alpha_t[:, None] * noised - sigma_t[:, None] * predicted
    weight = jnp.maximum(alpha_t * alpha_t / (sigma_t * sigma_t), 1.0)
    element_count = clean_latent.shape[0] * clean_latent.shape[1]
    slope_pred = -2.0 / element_count * (sigma_t * weight)[:, None] * (estimate - distill_target)
    back_norm = jnp.dot(slope_pred.reshape(row_count, CH), embed_out.astype(jnp.float32).T, precision=lax.Precision.HIGHEST)
    back_state = pullback(back_norm.reshape(samples, seq_len, model_width))[0]
    back_part = (gate_rows * back_state).astype(jnp.bfloat16).reshape(row_count, model_width)
    back_hidden = lax.dot_general(back_part, student_down, (((1,), (1,)), ((), ())), preferred_element_type=jnp.float32)
    back_pre = (back_hidden * gelu_slope(pre_act)).astype(jnp.bfloat16)
    grad_up = lax.dot_general(normed, back_pre, (((0,), (0,)), ((), ())), preferred_element_type=jnp.float32)
    grad_down = lax.dot_general(hidden, back_part, (((0,), (0,)), ((), ())), preferred_element_type=jnp.float32)
    return (distill_target, grad_up, grad_down)
```

```python
import functools
import math

import jax
import jax.numpy as jnp
from jax import lax
from jax.experimental import pallas as pl
from jax.experimental.pallas import tpu as pltpu
from jax.sharding import PartitionSpec as P


CH = 16
TSTEPS = 1000
STRIDE = 125
STEPS = 2
SECTION, DP = "section", "dp"
BOTH = (SECTION, DP)

norm_eps = 1e-06


def layer_norm(values):
    center = values - jnp.mean(values, axis=-1, keepdims=True)
    spread = jnp.mean(center * center, axis=-1, keepdims=True)
    return center * lax.rsqrt(spread + norm_eps)


def sinusoid(step_ids, model_width):
    half_width = model_width // 2
    frequency = jnp.exp(-math.log(10000.0) * jnp.arange(half_width, dtype=jnp.float32) / half_width)
    phase_arg = step_ids.astype(jnp.float32)[:, None] * frequency[None, :]
    return jnp.concatenate([jnp.cos(phase_arg), jnp.sin(phase_arg)], axis=-1)


def plan(step_ids):
    angle_t = 0.5 * math.pi / TSTEPS * step_ids.astype(jnp.float32)
    return (jnp.cos(angle_t), jnp.sin(angle_t))


def gelu_slope(pre_act):
    return jax.vjp(lambda inner: jax.nn.gelu(inner, approximate=True), pre_act)[1](
        jnp.ones_like(pre_act)
    )[0]


def flipped(block, axis, bit):
    return lax.ppermute(block, axis, [(i, i ^ (1 << bit)) for i in range(lax.axis_size(axis))])


def ordered(block, other, axis, bit):
    low = ((lax.axis_index(axis) >> bit) & 1) == 0
    return jnp.where(low, jnp.concatenate([block, other]), jnp.concatenate([other, block]))


def doubled(block, axis, bits):
    for bit in bits:
        other = flipped(block, axis, bit)
        block = ordered(block, other, axis, bit)
    return block


def layered(section_count, dp_count):
    return section_count == 4 and dp_count == 8


class Columns:
    def __init__(self, section_count, dp_count):
        self.sections, self.dps = section_count, dp_count
        self.planes = dp_count // 2

    def move(self, block, target, keep):
        pairs = []
        for s in range(self.sections):
            for d in range(self.dps):
                if keep(d // 2):
                    s2, d2 = target(s, d)
                    pairs.append((s * self.dps + d, s2 * self.dps + d2))
        return lax.ppermute(block, BOTH, pairs)

    def everywhere(self, plane):
        return True

    def inside(self, plane):
        return 0 < plane < self.planes - 1

    def x(self, block):
        return self.move(block, lambda s, d: (s ^ 2, d), self.everywhere)

    def y(self, block):
        return self.move(block, lambda s, d: (s, d ^ 1), self.everywhere)

    def core(self, block):
        return self.move(block, lambda s, d: (s ^ 1, d), self.everywhere)

    def beside(self, block):
        return self.move(block, lambda s, d: (s, d ^ 2), self.everywhere)

    def swap(self, block):
        last = self.planes - 1
        inner = lambda d: (last - d // 2) * 2 + d % 2
        target = lambda s, d: (s, inner(d)) if self.inside(d // 2) else (s ^ 1, d)
        return self.move(block, target, self.everywhere)

    def rows_of_all(self, block, after=lambda value: value):
        others = []
        for flip in range(1, self.planes):
            others.append(self.move(block, lambda s, d: (s, d ^ (2 * flip)), self.everywhere))
        others = after(tuple(others))
        block = ordered(block, others[0], DP, 1)
        block = ordered(block, ordered(others[1], others[2], DP, 1), DP, 2)
        other = self.y(block)
        low = lax.axis_index(DP) % 2 == 0
        pair = jnp.stack([jnp.where(low, block, other), jnp.where(low, other, block)])
        pair = pair.reshape((2, self.planes, block.shape[0] // self.planes) + block.shape[1:])
        return pair.swapaxes(0, 1).reshape((2 * block.shape[0],) + block.shape[1:])

    def endings(self, block):
        block = doubled(block, SECTION, [0])
        over_x = self.x(block)
        over_y = self.y(block)
        over_xy = self.move(block, lambda s, d: (s ^ 2, d ^ 1), self.everywhere)
        block = ordered(
            ordered(block, over_x, SECTION, 1), ordered(over_y, over_xy, SECTION, 1), DP, 0
        )
        beside = self.beside(block)
        swap = self.swap(block)
        far = self.move(block, lambda s, d: (s, d ^ 4), self.everywhere)
        plane = lax.axis_index(DP) // 2
        inside = (plane > 0) & (plane < self.planes - 1)
        near, other = jnp.where(inside, block, beside), jnp.where(inside, swap, far)
        return jnp.where(
            plane * 2 < self.planes, jnp.concatenate([near, other]), jnp.concatenate([other, near])
        )

    def total(self, partial, held):
        after = lambda value, mark: lax.optimization_barrier((value, mark))[0]
        total = partial
        for bit in range(2):
            half = total.shape[0] // 2
            at = (lax.axis_index(SECTION) >> bit) & 1
            kept = lax.dynamic_slice_in_dim(total, at * half, half, 0).astype(jnp.bfloat16)
            sent = lax.dynamic_slice_in_dim(total, (1 - at) * half, half, 0).astype(jnp.bfloat16)
            other = flipped(sent, SECTION, bit)
            total = kept.astype(jnp.float32) + other.astype(jnp.float32)
        block = total.astype(jnp.bfloat16)
        block = self.rows_of_all(block, lambda value: after(value, held["f"]))
        other = self.x(block)
        block = ordered(block, other, SECTION, 1)
        other = self.core(block)
        return [rows.reshape(2, self.dps, total.shape[0], total.shape[1]) for rows in (block, other)]

    def gather(self, own):
        held = {"n": own}

        def take(name, source, how):
            held[name] = how(held[source])

        take("x", "n", self.x)
        take("y", "n", self.y)
        take("s", "n", self.swap)
        take("o", "n", self.beside)
        take("ox", "x", self.beside)
        take("f", "o", self.swap)
        take("d", "x", self.y)
        take("sx", "s", self.x)
        take("sy", "s", self.y)
        take("oy", "y", self.beside)
        take("fx", "ox", self.swap)
        take("od", "d", self.beside)
        take("fy", "oy", self.swap)
        take("sd", "sy", self.x)
        take("fd", "fx", self.y)
        names = [plane + column for plane in ("", "o", "s", "f") for column in ("", "x", "y", "d")]
        names = [name or "n" for name in names]
        pieces = [held[name] for name in names]
        for name in names:
            pieces.append(self.core(held[name]))
        return pieces, held


def pack_kernel(up_ref, down_ref, piece_ref, sems):
    width = piece_ref.shape[1]
    rows = up_ref.shape[0]
    parts = up_ref.shape[1] // width
    copies = [
        pltpu.make_async_copy(
            up_ref.at[:, pl.ds(i * width, width)], piece_ref.at[pl.ds(i * rows, rows), :], sems.at[i]
        )
        for i in range(parts)
    ]
    copies.append(
        pltpu.make_async_copy(down_ref, piece_ref.at[pl.ds(parts * rows, down_ref.shape[0]), :], sems.at[parts])
    )
    for copy in copies:
        copy.start()
    for copy in copies:
        copy.wait()


def pack(up, down):
    width = down.shape[1]
    parts = up.shape[1] // width
    anywhere = pl.BlockSpec(memory_space=pl.ANY)
    return pl.pallas_call(
        pack_kernel,
        out_shape=jax.ShapeDtypeStruct((parts * up.shape[0] + down.shape[0], width), up.dtype),
        in_specs=[anywhere, anywhere],
        out_specs=pl.BlockSpec(memory_space=pltpu.VMEM),
        scratch_shapes=[pltpu.SemaphoreType.DMA((parts + 1,))],
    )(up, down)


def piece_loads(pieces, up_all, down_all, sems, layer):
    section_at, dp_at = lax.axis_index(SECTION), lax.axis_index(DP)
    plane_at, row_at = dp_at // 2, dp_at % 2
    width = up_all.shape[1]
    parts = up_all.shape[2] // width
    up_rows = pieces[0].shape[0] // (2 * parts)
    down_rows = parts * up_rows
    last = width // up_rows // 2 - 1
    beside = plane_at ^ 1
    planes = [plane_at, beside, last - plane_at, last - beside]
    for core_flip in range(2):
        for x_flip in range(2):
            held = section_at ^ (2 * x_flip + core_flip)

            @pl.when(held == layer)
            def _():
                for plane_kind in range(4):
                    for y_flip in range(2):
                        piece = pieces[core_flip * 16 + plane_kind * 4 + y_flip * 2 + x_flip]
                        shard = planes[plane_kind] * 2 + (row_at ^ y_flip)
                        slot = plane_kind * 2 + y_flip
                        up_span = pl.ds(pl.multiple_of(shard * up_rows, 16), up_rows)
                        down_span = pl.ds(pl.multiple_of(shard * down_rows, 16), down_rows)
                        for part in range(parts):
                            pltpu.make_async_copy(
                                piece.at[pl.ds(part * up_rows, up_rows), :],
                                up_all.at[layer, up_span, pl.ds(part * width, width)],
                                sems.at[part, layer, slot],
                            ).start()
                        pltpu.make_async_copy(
                            piece.at[pl.ds(down_rows, down_rows), :],
                            down_all.at[layer, down_span, :],
                            sems.at[parts, layer, slot],
                        ).start()


def piece_waits(pieces, up_all, down_all, sems, layer):
    width = up_all.shape[1]
    parts = up_all.shape[2] // width
    up_rows = pieces[0].shape[0] // (2 * parts)
    down_rows = parts * up_rows
    for slot in range(8):
        for part in range(parts):
            pltpu.make_async_copy(
                pieces[0].at[pl.ds(0, up_rows), :],
                up_all.at[layer, pl.ds(slot * up_rows, up_rows), pl.ds(part * width, width)],
                sems.at[part, layer, slot],
            ).wait()
        pltpu.make_async_copy(
            pieces[0].at[pl.ds(down_rows, down_rows), :],
            down_all.at[layer, pl.ds(slot * down_rows, down_rows), :],
            sems.at[parts, layer, slot],
        ).wait()


def whole_copies(pieces, up_all, down_all, sems, layer):
    last = sems.shape[0] - 1
    return [
        pltpu.make_async_copy(pieces[0].at[layer], up_all.at[layer], sems.at[0, layer, 0]),
        pltpu.make_async_copy(pieces[1].at[layer], down_all.at[layer], sems.at[last, layer, 0]),
    ]


def teacher_kernel(count, piecewise, latent_ref, cond_ref, coef_ref, gain_ref, bias_ref, in_ref, out_ref, *rest):
    pieces = rest[:count]
    final_ref, up_all, down_all, state, latent, sems = rest[count:]
    layers = up_all.shape[0]
    model_width = in_ref.shape[1]
    groups = cond_ref.shape[1]
    tokens = latent_ref.shape[0]
    rows = 2 * tokens
    seq_len = rows // groups

    @pl.loop(0, layers)
    def _(layer):
        if piecewise:
            piece_loads(pieces, up_all, down_all, sems, layer)
        else:
            for copy in whole_copies(pieces, up_all, down_all, sems, layer):
                copy.start()

    def enter(values):
        entry = jnp.dot(values.astype(jnp.bfloat16), in_ref[...], preferred_element_type=jnp.float32)
        entry = entry.astype(jnp.bfloat16)
        state[:tokens] = entry
        state[tokens:] = entry

    latent[...] = latent_ref[...]
    enter(latent[...])

    @pl.loop(0, STEPS)
    def _(step):
        @pl.loop(0, layers)
        def _(layer):
            @pl.when(step == 0)
            def _():
                if piecewise:
                    piece_waits(pieces, up_all, down_all, sems, layer)
                else:
                    for copy in whole_copies(pieces, up_all, down_all, sems, layer):
                        copy.wait()

            cond = cond_ref[step]
            gain, bias = gain_ref[layer], bias_ref[layer]
            shift, scale, gate = [
                (cond * gain[i : i + 1] + bias[i : i + 1])[:, None, :] for i in range(3)
            ]
            normed = layer_norm(state[...].astype(jnp.float32)).reshape(groups, seq_len, model_width)
            normed = (normed * (1.0 + scale) + shift).astype(jnp.bfloat16).reshape(rows, model_width)
            pre_act = jnp.dot(normed, up_all[layer], preferred_element_type=jnp.float32)
            hidden = jax.nn.gelu(pre_act, approximate=True).astype(jnp.bfloat16)
            mixed = jnp.dot(hidden, down_all[layer], preferred_element_type=jnp.float32)
            residual = state[...].astype(jnp.float32).reshape(groups, seq_len, model_width)
            result = residual + gate * mixed.reshape(groups, seq_len, model_width)
            state[...] = result.astype(jnp.bfloat16).reshape(rows, model_width)

        normed = layer_norm(state[...].astype(jnp.float32)).astype(jnp.bfloat16)
        predicted = jnp.dot(normed, out_ref[...], preferred_element_type=jnp.float32)
        coef = coef_ref[step]
        guided = coef[:, 0:1] * predicted[:tokens] - coef[:, 1:2] * predicted[tokens:]
        latent[...] = coef[:, 2:3] * latent[...] + coef[:, 3:4] * guided
        enter(latent[...])

    final_ref[...] = latent[...]


def run_teacher(latent, cond, coef, gain, bias, embed_in, embed_out, pieces, hidden, piecewise):
    layers, model_width = gain.shape[0], embed_in.shape[1]
    parts = hidden // model_width
    vmem, anywhere = pl.BlockSpec(memory_space=pltpu.VMEM), pl.BlockSpec(memory_space=pl.ANY)
    rows = 2 * latent.shape[0]
    return pl.pallas_call(
        functools.partial(teacher_kernel, len(pieces), piecewise),
        out_shape=jax.ShapeDtypeStruct(latent.shape, jnp.float32),
        in_specs=[vmem] * 7 + [anywhere] * len(pieces),
        out_specs=vmem,
        scratch_shapes=[
            pltpu.VMEM((layers, model_width, hidden), jnp.bfloat16),
            pltpu.VMEM((layers, hidden, model_width), jnp.bfloat16),
            pltpu.VMEM((rows, model_width), jnp.bfloat16),
            pltpu.VMEM(latent.shape, jnp.float32),
            pltpu.SemaphoreType.DMA((parts + 1, layers, 8)),
        ],
        compiler_params=pltpu.CompilerParams(vmem_limit_bytes=60 * 1024 * 1024),
        cost_estimate=pl.CostEstimate(
            flops=4 * STEPS * layers * rows * model_width * hidden,
            bytes_accessed=4 * layers * model_width * hidden,
            transcendentals=0,
        ),
    )(latent, cond, coef, gain, bias, embed_in, embed_out, *pieces)


def student_kernel(own_ref, other_ref, tokens_ref, gate_ref, in_ref, out_ref, unit_ref, inverse_ref, predicted_ref):
    rows, model_width = unit_ref.shape
    samples = gate_ref.shape[0]
    residual = jnp.dot(tokens_ref[...], in_ref[...], preferred_element_type=jnp.float32)
    residual = residual.astype(jnp.bfloat16).astype(jnp.float32)
    groups = own_ref.shape[1]
    first = lax.axis_index(SECTION) % 2 == 0
    mixed = []
    for i in range(groups):
        own = own_ref[:, i].reshape(rows // groups // 2, model_width).astype(jnp.float32)
        other = other_ref[:, i].reshape(rows // groups // 2, model_width).astype(jnp.float32)
        mixed += [jnp.where(first, own, other), jnp.where(first, other, own)]
    mixed = jnp.concatenate(mixed)
    by_sample = lambda values: values.reshape(samples, rows // samples, model_width)
    state = by_sample(residual) + gate_ref[...][:, None, :] * by_sample(mixed)
    state = state.reshape(rows, model_width)
    center = state - jnp.mean(state, axis=-1, keepdims=True)
    inverse = lax.rsqrt(jnp.mean(center * center, axis=-1, keepdims=True) + norm_eps)
    unit = (center * inverse).astype(jnp.bfloat16)
    unit_ref[...] = unit
    inverse_ref[...] = inverse
    predicted_ref[...] = jnp.dot(unit, out_ref[...], preferred_element_type=jnp.float32)


def run_student(halves, tokens, gate, embed_in, embed_out):
    rows, model_width = tokens.shape[0], embed_in.shape[1]
    held = halves[0].shape
    groups = min(2, held[1])
    block = rows // held[1] * groups
    samples = gate.shape[0] * block // rows
    by_rows = lambda columns: pl.BlockSpec((block, columns), lambda i: (i, 0))
    whole = lambda values: pl.BlockSpec(values.shape, lambda i: (0, 0))
    return pl.pallas_call(
        student_kernel,
        grid=(rows // block,),
        out_shape=[
            jax.ShapeDtypeStruct((rows, model_width), jnp.bfloat16),
            jax.ShapeDtypeStruct((rows, 1), jnp.float32),
            jax.ShapeDtypeStruct((rows, CH), jnp.float32),
        ],
        in_specs=[
            pl.BlockSpec((held[0], groups) + held[2:], lambda i: (0, i, 0, 0)),
            pl.BlockSpec((held[0], groups) + held[2:], lambda i: (0, i, 0, 0)),
            by_rows(CH),
            pl.BlockSpec((samples, model_width), lambda i: (i, 0)),
            whole(embed_in),
            whole(embed_out),
        ],
        out_specs=[by_rows(model_width), by_rows(1), by_rows(CH)],
        compiler_params=pltpu.CompilerParams(dimension_semantics=("arbitrary",)),
        cost_estimate=pl.CostEstimate(
            flops=64 * rows * model_width, bytes_accessed=8 * rows * model_width, transcendentals=0
        ),
    )(*halves, tokens, gate, embed_in, embed_out)


def gradient_kernel(
    unit_ref, inverse_ref, predicted_ref, gate_ref, slope_ref, lead_ref, coef_ref, wide_ref, down_ref, normed_ref,
    hidden_ref, grad_up_ref, grad_down_ref, back_part, back_pre,
):
    step = pl.program_id(0)
    rows, model_width = unit_ref.shape
    samples = gate_ref.shape[0]
    predicted = predicted_ref[...]
    cotangent = inverse_ref[...] * (lead_ref[...] - coef_ref[...] * predicted)
    mean_out = jnp.mean(wide_ref[...].astype(jnp.float32), axis=1)[None]
    first_mean = jnp.sum(cotangent * mean_out, axis=1, keepdims=True)
    second_mean = jnp.sum(cotangent * predicted, axis=1, keepdims=True) * (1.0 / model_width)
    high = cotangent.astype(jnp.bfloat16)
    low = cotangent - high.astype(jnp.float32)
    middle = low.astype(jnp.bfloat16)
    low = (low - middle.astype(jnp.float32)).astype(jnp.bfloat16)
    wide = wide_ref[...]
    back_norm = jnp.dot(
        jnp.concatenate([high, middle, low], axis=1),
        jnp.concatenate([wide, wide, wide]),
        preferred_element_type=jnp.float32,
    )
    unit = unit_ref[...].astype(jnp.float32)
    back_state = back_norm - first_mean - unit * second_mean
    back_state = back_state.reshape(samples, rows // samples, model_width)
    part = (gate_ref[...][:, None, :] * back_state).reshape(rows, model_width).astype(jnp.bfloat16)
    here = pl.ds(pl.multiple_of(step * rows, rows), rows)
    back_part[here, :] = part
    back_hidden = jnp.dot(part, down_ref[...], preferred_element_type=jnp.float32)
    back_pre[here, :] = (back_hidden * slope_ref[...]).astype(jnp.bfloat16)

    @pl.when(step == pl.num_programs(0) - 1)
    def _():
        contract_rows = (((0,), (0,)), ((), ()))
        grad_up_ref[...] = lax.dot_general(
            normed_ref[...], back_pre[...], contract_rows, preferred_element_type=jnp.float32
        )
        grad_down_ref[...] = lax.dot_general(
            hidden_ref[...], back_part[...], contract_rows, preferred_element_type=jnp.float32
        )


def run_gradient(unit, inverse, predicted, gate, slope, lead, coef, embed_out, down, normed, hidden):
    rows, hidden_local = slope.shape
    model_width = unit.shape[1]
    block = rows // 4
    samples = gate.shape[0] * block // rows
    wide_out = embed_out.T
    by_rows = lambda columns: pl.BlockSpec((block, columns), lambda i: (i, 0))
    whole = lambda values: pl.BlockSpec(values.shape, lambda i: (0, 0))
    grads = [
        jax.ShapeDtypeStruct((normed.shape[1], hidden_local), jnp.float32),
        jax.ShapeDtypeStruct((hidden.shape[1], model_width), jnp.float32),
    ]
    return pl.pallas_call(
        gradient_kernel,
        grid=(rows // block,),
        out_shape=grads,
        in_specs=[
            by_rows(model_width),
            by_rows(1),
            by_rows(CH),
            pl.BlockSpec((samples, model_width), lambda i: (i, 0)),
            by_rows(hidden_local),
            by_rows(CH),
            by_rows(1),
        ]
        + [whole(v) for v in (wide_out, down, normed, hidden)],
        out_specs=[whole(grads[0]), whole(grads[1])],
        scratch_shapes=[
            pltpu.VMEM((rows, model_width), jnp.bfloat16),
            pltpu.VMEM((rows, hidden_local), jnp.bfloat16),
        ],
        compiler_params=pltpu.CompilerParams(
            dimension_semantics=("arbitrary",), vmem_limit_bytes=60 * 1024 * 1024
        ),
        cost_estimate=pl.CostEstimate(
            flops=3 * rows * model_width * hidden_local, bytes_accessed=12 * rows * model_width, transcendentals=0
        ),
    )(unit, inverse, predicted, gate, slope, lead, coef, wide_out, down, normed, hidden)


def body(
    clean_latent,
    noise_draw,
    step_index,
    labels,
    guide_level,
    class_table,
    embed_in,
    embed_out,
    teacher_up,
    teacher_down,
    teacher_gain,
    teacher_bias,
    student_up,
    student_down,
    student_gain,
    student_bias,
    guide_vec,
):
    section_count, dp_count = lax.axis_size(SECTION), lax.axis_size(DP)
    section_at, dp_at = lax.axis_index(SECTION), lax.axis_index(DP)
    own_samples, latent_width = clean_latent.shape
    samples = own_samples * dp_count
    seq_len = latent_width // CH
    model_width = class_table.shape[1]
    hidden_local = student_up.shape[1]
    columns = Columns(section_count, dp_count) if layered(section_count, dp_count) else None
    dp_bits = range(dp_count.bit_length() - 1)
    section_bits = range(section_count.bit_length() - 1)

    hidden_width = teacher_up.shape[2]
    if columns is not None:
        pieces, held = columns.gather(pack(teacher_up[0], teacher_down[0]))
    else:
        full_up = lax.all_gather(teacher_up[0], DP, axis=0, tiled=True)
        full_down = lax.all_gather(teacher_down[0], DP, axis=0, tiled=True)
        pieces = [lax.all_gather(full_up, SECTION, axis=0), lax.all_gather(full_down, SECTION, axis=0)]
    gain = doubled(jnp.concatenate([teacher_gain, teacher_bias], axis=1), SECTION, section_bits)
    gain, bias = gain[:, :3], gain[:, 3:]

    scalars = jnp.stack([step_index, labels, guide_level], axis=1).astype(jnp.float32)
    shared = jnp.concatenate([clean_latent, noise_draw, jnp.pad(scalars, ((0, 0), (0, 125)))], axis=1)
    if columns is not None:
        shared = columns.rows_of_all(shared)
    else:
        shared = doubled(shared, DP, dp_bits)
    clean_all, noise_all = shared[:, :latent_width], shared[:, latent_width : 2 * latent_width]
    scalars = shared[:, 2 * latent_width : 2 * latent_width + 3].astype(jnp.int32)
    step_all, label_all, level_all = scalars[:, 0], scalars[:, 1], scalars[:, 2]
    guidance = 0.5 * level_all.astype(jnp.float32)
    alpha_all, sigma_all = plan(step_all)
    alpha_end, sigma_end = plan(step_all - STEPS * STRIDE)
    noised = alpha_all[:, None] * clean_all + sigma_all[:, None] * noise_all

    teachers = section_count * (dp_count // 2 if columns is not None else dp_count)
    per_device = samples // teachers
    if columns is not None:
        position = jnp.clip(dp_at - 2, 0, dp_count // 2 - 1) * section_count + section_at
    else:
        position = dp_at * section_count + section_at
    first = position * per_device
    pick = lambda values: lax.dynamic_slice_in_dim(values, first, per_device, 0)
    own_steps, own_labels, own_weight = pick(step_all), pick(label_all), pick(guidance)
    label_rows = jnp.take(class_table, own_labels, axis=0).astype(jnp.float32)
    null_row = class_table[class_table.shape[0] - 1].astype(jnp.float32)
    cond, coef = [], []
    for step in range(STEPS):
        time_now = own_steps - step * STRIDE
        wave = sinusoid(time_now, model_width)
        cond.append(jnp.concatenate([wave + label_rows, wave + null_row[None]]))
        alpha_now, sigma_now = plan(time_now)
        alpha_next, sigma_next = plan(time_now - STRIDE)
        coef.append(
            jnp.stack(
                [
                    1.0 + own_weight,
                    own_weight,
                    alpha_next * alpha_now + sigma_next * sigma_now,
                    sigma_next * alpha_now - alpha_next * sigma_now,
                ],
                axis=1,
            )
        )
    coef = jnp.repeat(jnp.stack(coef), seq_len, axis=1)
    own_latent = pick(noised).reshape(per_device * seq_len, CH)
    wide = columns is not None
    own = lambda values: lax.dynamic_slice_in_dim(values, dp_at * own_samples, own_samples, 0)
    near = (lambda values: values) if wide else own
    local = near(noised)
    count = local.shape[0]
    rows = count * seq_len
    step_at, weight_at = near(step_all), near(guidance)
    alpha_at, sigma_at = near(alpha_all), near(sigma_all)
    student_cond = (
        sinusoid(step_at, model_width)
        + jnp.take(class_table, near(label_all), axis=0).astype(jnp.float32)
        + weight_at[:, None] * guide_vec[None, :]
    )
    modulation = student_cond[:, None, :] * student_gain[None] + student_bias[None]
    shift, scale, gate = [modulation[:, i, None, :] for i in range(3)]
    tokens_in = local.reshape(rows, CH).astype(jnp.bfloat16)
    tokens = jnp.dot(tokens_in, embed_in, preferred_element_type=jnp.float32)
    residual = tokens.astype(jnp.bfloat16).astype(jnp.float32).reshape(count, seq_len, model_width)
    normed = (layer_norm(residual) * (1.0 + scale) + shift).astype(jnp.bfloat16).reshape(rows, model_width)
    pre_act = jnp.dot(normed, student_up, preferred_element_type=jnp.float32)
    hidden = jax.nn.gelu(pre_act, approximate=True).astype(jnp.bfloat16)
    slope = gelu_slope(pre_act)
    own_rows = own_samples * seq_len
    own_hidden = lax.dynamic_slice_in_dim(hidden, dp_at * own_rows, own_rows, 0) if wide else hidden
    partial = jnp.dot(own_hidden, student_down, preferred_element_type=jnp.float32)
    weight = jnp.maximum(alpha_at * alpha_at / (sigma_at * sigma_at), 1.0)
    factor = -2.0 / (samples * latent_width) * (sigma_at * weight)[:, None]
    if wide:
        hidden_rows = hidden_local // dp_count
        width_rows = model_width // dp_count
        hidden = lax.dynamic_slice_in_dim(hidden, dp_at * hidden_rows, hidden_rows, 1)
        normed = lax.dynamic_slice_in_dim(normed, dp_at * width_rows, width_rows, 1)
        turned_down = student_down.T
        summed = columns.total(partial, held)
        student = run_student(summed, tokens_in, modulation[:, 2], embed_in, embed_out)
        own_latent, normed, hidden, slope, turned_down, student = lax.optimization_barrier(
            (own_latent, normed, hidden, slope, turned_down, student)
        )

    raw_ending = run_teacher(
        own_latent, jnp.stack(cond), coef, gain, bias, embed_in, embed_out, pieces, hidden_width, columns is not None
    ).reshape(per_device, latent_width)
    if columns is not None:
        ending = columns.endings(raw_ending)
    else:
        ending = doubled(doubled(raw_ending, SECTION, section_bits), DP, dp_bits)
    ratio = sigma_end / sigma_all
    target_all = (ending - ratio[:, None] * noised) / (alpha_end - ratio * alpha_all)[:, None]
    distill_target = lax.dynamic_slice_in_dim(target_all, dp_at * own_samples, own_samples, 0)

    if wide:
        lead = (factor * (alpha_at[:, None] * local - target_all)).reshape(rows, CH)
        grad_up, grad_down = run_gradient(
            *student,
            modulation[:, 2],
            slope,
            lead,
            jnp.repeat(factor * sigma_at[:, None], seq_len, axis=0),
            embed_out,
            turned_down,
            normed,
            hidden,
        )
        return (distill_target, grad_up, grad_down)
    target_at = own(target_all)
    mixed = lax.psum(partial.astype(jnp.bfloat16), SECTION)
    state = residual + gate * mixed.astype(jnp.float32).reshape(count, seq_len, model_width)
    center = state - jnp.mean(state, axis=-1, keepdims=True)
    inverse = lax.rsqrt(jnp.mean(center * center, axis=-1, keepdims=True) + norm_eps)
    unit = center * inverse
    unit_rows = unit.reshape(rows, model_width)
    predicted = jnp.dot(unit_rows.astype(jnp.bfloat16), embed_out, preferred_element_type=jnp.float32)
    estimate = alpha_at[:, None] * local - sigma_at[:, None] * predicted.reshape(count, latent_width)
    wide_out = embed_out.astype(jnp.float32)
    projected = jnp.dot(unit_rows, wide_out, precision=lax.Precision.HIGHEST) / model_width
    mean_out = jnp.mean(wide_out, axis=0)
    lead = (gate * inverse).reshape(rows, model_width)
    pull = lead * unit_rows
    cotangent = (factor * (estimate - target_at)).reshape(rows, CH)
    first_mean = jnp.sum(cotangent * mean_out[None], axis=1, keepdims=True)
    second_mean = jnp.sum(cotangent * projected, axis=1, keepdims=True)
    back_norm = jnp.dot(cotangent, wide_out.T, precision=lax.Precision.HIGHEST)
    back_part = (lead * (back_norm - first_mean) - pull * second_mean).astype(jnp.bfloat16)
    back_hidden = lax.dot_general(
        back_part, student_down, (((1,), (1,)), ((), ())), preferred_element_type=jnp.float32
    )
    back_pre = (back_hidden * slope).astype(jnp.bfloat16)
    contract_rows = (((0,), (0,)), ((), ()))
    grad_up = lax.dot_general(normed, back_pre, contract_rows, preferred_element_type=jnp.float32)
    grad_down = lax.dot_general(hidden, back_part, contract_rows, preferred_element_type=jnp.float32)
    grad_up = lax.psum_scatter(grad_up, DP, scatter_dimension=0, tiled=True)
    grad_down = lax.psum_scatter(grad_down, DP, scatter_dimension=0, tiled=True)
    return (distill_target, grad_up, grad_down)


def solution(mesh):
    return jax.shard_map(
        body,
        mesh=mesh,
        in_specs=(
            P(DP, None),
            P(DP, None),
            P(DP),
            P(DP),
            P(DP),
            P(),
            P(),
            P(),
            P(SECTION, DP, None),
            P(SECTION, DP, None),
            P(SECTION, None, None),
            P(SECTION, None, None),
            P(None, SECTION),
            P(SECTION, None),
            P(),
            P(),
            P(),
        ),
        out_specs=(P(DP, None), P(DP, SECTION), P((SECTION, DP), None)),
        check_vma=False,
    )
```
